256 devices in a mesh: row: 32 (over y, z), col: 8 (over x, core).
Axes of the slice: x: 4, y: 4, z: 8, core: 2. Of those that a mesh axis runs over, the one named last changes fastest.
Arguments:
- valence: bfloat16 [131072, 2048], P('row', 'col')
- conduction: bfloat16 [131072, 1024], P('row', 'col')
- point_index: int32 [8192], replicated, may hold values from 0 to 131071, as said below
Outputs:
- gram: float32 [8192, 8192], P('col', 'row')
The draws below stay inside these ranges and needn't reach their ends.
Inputs may be any that keep to these rules, and one draw needn't show every extreme that they name: `point_index`: 8192 distinct cells; cell g lies in slab g // 4096. In each aligned block of 256 entries, at most 16 lie in any one slab, and in every block some slab holds exactly 16.
All inputs are finite; a program needn't handle non-finite values.
Results may differ from the reference program's by a relative error of at most 0.0003.
Values may be sent and summed in bfloat16 or wider, within the bound.
No kernel may reach another device: no remote copies, remote signals or barrier semaphores. Data moves between devices by JAX's collectives and lax.ppermute only.
A program may use at most 128 MiB of HBM per device.

```python
import jax
import jax.numpy as jnp
from jax import lax

NV = 2048
NC = 1024
NP = 8192
GRID_DEV = 4096
PR = 256
CAP = 16
N_ROW = 32


mode_count = 16


def orbital_draw(key, rows, bands):
    noise_key, coef_key, mode_key = jax.random.split(key, 3)
    noise = jax.random.normal(noise_key, (rows, bands), jnp.float32)
    coefs = 0.5 * jax.random.normal(coef_key, (rows, mode_count), jnp.float32)
    modes = jax.random.normal(mode_key, (mode_count, bands), jnp.float32)
    values = (noise + jnp.dot(coefs, modes)) / jnp.sqrt(5.0 * bands)
    return values.astype(jnp.bfloat16)


def draw_valence(key, part):
    return orbital_draw(key, GRID_DEV * N_ROW, NV)


def draw_conduction(key, part):
    return orbital_draw(jax.random.fold_in(key, 11), GRID_DEV * N_ROW, NC)


def draw_point_index(key, part):
    slots = N_ROW * CAP
    score_key, favor_key, cell_key, order_key = jax.random.split(key, 4)
    scores = jax.random.randint(score_key, (N_ROW, slots), 0, 1 << 16) * slots
    scores = scores + jnp.arange(slots, dtype=jnp.int32)[None, :]
    favored = jax.random.randint(favor_key, (N_ROW,), 0, N_ROW)
    slot_slab = jnp.arange(slots, dtype=jnp.int32) // CAP
    scores = scores + jnp.where(slot_slab[None, :] == favored[:, None], 1 << 29, 0)
    chosen = lax.top_k(scores, PR)[1].astype(jnp.int32)
    slab = chosen // CAP
    within = chosen - slab * CAP
    perms = jax.vmap(lambda k: jax.random.permutation(k, GRID_DEV))(jax.random.split(cell_key, N_ROW)).astype(jnp.int32)
    block_ids = jnp.arange(N_ROW, dtype=jnp.int32)[:, None]
    local = perms[slab, block_ids * CAP + within]
    cells = slab * GRID_DEV + local
    orders = jax.vmap(lambda k: jax.random.permutation(k, PR))(jax.random.split(order_key, N_ROW)).astype(jnp.int32)
    cells = jnp.take_along_axis(cells, orders, axis=1)
    return cells.reshape(NP).astype(jnp.int32)


def setup_inputs(seed: int = 0) -> dict:
    key_of = jax.random.split(jax.random.key(seed), 4)
    return {
        "valence": draw_valence(jax.random.fold_in(key_of[3], 71), 0),
        "conduction": draw_conduction(jax.random.fold_in(key_of[3], 71), 0),
        "point_index": draw_point_index(jax.random.fold_in(key_of[3], 71), 0),
    }


def full_total(rows, cols):
    left = rows.astype(jnp.float32)
    right = cols.astype(jnp.float32)
    return jnp.dot(left, right.T, precision=lax.Precision.HIGHEST)


def reference(valence, conduction, point_index):
    psi_mu = jnp.take(valence, point_index, axis=0)
    phi_mu = jnp.take(conduction, point_index, axis=0)
    psi_blocks = psi_mu.reshape(NP // PR, PR, NV)
    phi_blocks = phi_mu.reshape(NP // PR, PR, NC)

    def one_block(pair):
        return full_total(pair[0], psi_mu) * full_total(pair[1], phi_mu)

    stacked = lax.map(one_block, (psi_blocks, phi_blocks))
    return stacked.reshape(NP, NP)
```

```python
import jax
import jax.numpy as jnp
from jax import lax
from jax.experimental import pallas as pl
from jax.experimental.pallas import tpu as pltpu
from jax.sharding import Mesh, PartitionSpec as P


NY, NZ, NX, NK = 4, 8, 4, 2
AXES = ("y", "z", "x", "core")
CAP = 16
RING = (0, -1, 1, 2)


def route(where):
    pairs = []
    for y in range(NY):
        for z in range(NZ):
            for x in range(NX):
                for k in range(NK):
                    ty, tz, tx, tk = where(y, z, x, k)
                    src = ((y * NZ + z) * NX + x) * NK + k
                    dst = ((ty % NY * NZ + tz % NZ) * NX + tx % NX) * NK + tk % NK
                    pairs.append((src, dst))
    return pairs


def send(a, where):
    return lax.ppermute(a, AXES, route(where))


def first_ring(d):
    return lambda y, z, x, k: (y, z, x + d, k) if k == 0 else (y + d, z, x, k)


def second_ring(d):
    return lambda y, z, x, k: (y + d, z, x, k) if k == 0 else (y, z, x + d, k)


def z_ring(d):
    return lambda y, z, x, k: (y, z + d, x, k)


def y_ring(d):
    return lambda y, z, x, k: (y + d, z, x, k)


def other_core(y, z, x, k):
    return (y, z, x, 1 - k)


def to_left_owner(y, z, x, k):
    return (y, z ^ (2 * x + k), (y - z) % NY, z // 4)


def gather_plane(piece):
    minus, plus = send(piece, first_ring(1)), send(piece, first_ring(-1))
    across = send(piece, first_ring(2))
    mine = jnp.stack([piece, minus, plus, across])
    theirs = send(mine, other_core)
    m, p = send(mine, second_ring(1)), send(mine, second_ring(-1))
    fm, fp = send(m[:2], second_ring(1)), send(p[2:], second_ring(-1))
    handed = [send(a, other_core) for a in (m, p, fm, fp)]
    return [mine, m, p, fm, fp], [theirs, *handed]


def gather_column(piece):
    half = piece.shape[0] // 2
    out = [piece]
    m, p = piece, piece
    for _ in range(3):
        m, p = send(m, z_ring(1)), send(p, z_ring(-1))
        out += [m, p]
    out += [send(m[:half], z_ring(1)), send(p[half:], z_ring(-1))]
    return out


def gram_kernel(*refs):
    left, refs = refs[:9], refs[9:]
    bundles, refs = (refs[:5], refs[5:10]), refs[10:]
    outs, (lv, lc, rv, rc) = refs[:4], refs[4:]
    y, z, x, k = (lax.axis_index(a) for a in AXES)
    rows = left[0].shape[0]
    nv = rv.shape[1] // (NX * NK)
    nc = rc.shape[1] // (NX * NK)
    half = rows // 2
    zb = 4 * k + ((y - x) & 3)

    def cols(share, width):
        return pl.ds(pl.multiple_of(share * width, width), width)

    for ref, far, at in zip(
        left, (0, -1, 1, -2, 2, -3, 3, 4, 4), (0, 0, 0, 0, 0, 0, 0, 0, half)
    ):
        share = ((z + far) & 7) ^ zb
        here = pl.ds(at, ref.shape[0])
        lv[here, cols(share, nv)] = ref[:, :nv]
        lc[here, cols(share, nc)] = ref[:, nv:]
    for bundle, core in zip(bundles, (k, 1 - k)):
        for i, a in enumerate(RING):
            for j, b in enumerate(RING):
                if i < 3:
                    ref = bundle[i].at[j]
                else:
                    ref = bundle[3 + j // 2].at[j % 2]
                dy = jnp.where(core == 0, a, b) & 3
                dx = jnp.where(core == 0, b, a)
                share = 2 * ((x + dx) & 3) + core
                here = pl.ds(pl.multiple_of(dy * rows, rows), rows)
                rv[here, cols(share, nv)] = ref[:, :nv]
                rc[here, cols(share, nc)] = ref[:, nv:]
    dims = (((1,), (1,)), ((), ()))
    for e, out in enumerate(outs):
        here = pl.ds(pl.multiple_of(((e + z) & 3) * rows, rows), rows)
        gv = lax.dot_general(lv[...], rv[here, :], dims, preferred_element_type=jnp.float32)
        gc = lax.dot_general(lc[...], rc[here, :], dims, preferred_element_type=jnp.float32)
        out[...] = gv * gc


def gram_tiles(left, mine, theirs, nv):
    rows, width = left[0].shape
    nc = width - nv
    shares = NX * NK
    vmem = pl.BlockSpec(memory_space=pltpu.VMEM)
    return pl.pallas_call(
        gram_kernel,
        out_shape=[jax.ShapeDtypeStruct((rows, rows), jnp.float32)] * NY,
        in_specs=[vmem] * 19,
        out_specs=[vmem] * NY,
        scratch_shapes=[
            pltpu.VMEM((rows, shares * nv), jnp.bfloat16),
            pltpu.VMEM((rows, shares * nc), jnp.bfloat16),
            pltpu.VMEM((NY * rows, shares * nv), jnp.bfloat16),
            pltpu.VMEM((NY * rows, shares * nc), jnp.bfloat16),
        ],
        name="gram_tiles",
    )(*left, *mine, *theirs)


def place_kernel(*refs):
    parts, out = refs[:NY], refs[NY]
    y, x = lax.axis_index("y"), lax.axis_index("x")
    rows = parts[0].shape[0]
    for e, ref in enumerate(parts):
        out[pl.ds(pl.multiple_of(((y + e - x) & 3) * rows, rows), rows), :] = ref[...]


def place(parts):
    rows, width = parts[0].shape
    vmem = pl.BlockSpec(memory_space=pltpu.VMEM)
    return pl.pallas_call(
        place_kernel,
        out_shape=jax.ShapeDtypeStruct((NY * rows, width), jnp.float32),
        in_specs=[vmem] * NY,
        out_specs=vmem,
        name="place",
    )(*parts)


def on_device(valence, conduction, point_index):
    n_row = NY * NZ
    y, z = lax.axis_index("y"), lax.axis_index("z")
    my_row = y * NZ + z
    my_block = ((y - z) & 3) * NZ + z
    cells = valence.shape[0]
    blocks = point_index.reshape(n_row, -1)
    per_block = blocks.shape[1]
    owners = blocks // cells
    offsets = blocks - owners * cells
    at = jnp.arange(per_block, dtype=jnp.int32)
    earlier = (at[:, None] < at[None, :]).astype(jnp.bfloat16)
    owned = owners == my_row
    own_owner = lax.dynamic_index_in_dim(owners, my_block, 0, keepdims=False)
    own_is = own_owner[None, :] == jnp.arange(n_row, dtype=jnp.int32)[:, None]
    counts = jnp.dot(
        jnp.concatenate([owned, own_is]).astype(jnp.bfloat16),
        earlier,
        preferred_element_type=jnp.float32,
    ).astype(jnp.int32)
    ranks, own_ranks = counts[:n_row], counts[n_row:]
    slots = jnp.arange(CAP, dtype=jnp.int32)
    picked = owned[:, None, :] & (ranks[:, None, :] == slots[None, :, None])
    source = jnp.sum(jnp.where(picked, offsets[:, None, :], 0), axis=2)
    order = jnp.array(
        [((d // NZ - d % NZ) % NY) * NZ + d % NZ for d in range(n_row)], dtype=jnp.int32
    )
    source = source[order].reshape(-1)
    flat_slot = own_owner * CAP + jnp.sum(jnp.where(own_is, own_ranks, 0), axis=0)

    outgoing = jnp.concatenate([valence[source], conduction[source]], axis=1)
    got = lax.all_to_all(
        outgoing.reshape(n_row, CAP, -1), ("y", "z"), split_axis=0, concat_axis=0, tiled=True
    )
    piece = got.reshape(n_row * CAP, -1)[flat_slot]

    left = gather_column(send(piece, to_left_owner))
    mine, theirs = gather_plane(piece)
    tiles = gram_tiles(left, mine, theirs, valence.shape[1])
    parts = [tiles[0]] + [send(tiles[(-e) % NY], y_ring(-e)) for e in range(1, NY)]
    return place(parts)


def solution(mesh):
    fine = Mesh(mesh.devices.reshape(NY, NZ, NX, NK), AXES)
    row, col = ("y", "z"), ("x", "core")
    return jax.shard_map(
        on_device,
        mesh=fine,
        in_specs=(P(row, col), P(row, col), P()),
        out_specs=P(col, row),
        check_vma=False,
    )
```

```python
import functools

import jax
import jax.numpy as jnp
from jax import lax
from jax.experimental import pallas as pl
from jax.experimental.pallas import tpu as pltpu
from jax.sharding import Mesh, PartitionSpec as P


NY, NZ, NX, NK = 4, 8, 4, 2
AXES = ("y", "z", "x", "core")
CAP = 16
RING = (0, -1, 1, 2)


def route(where):
    pairs = []
    for y in range(NY):
        for z in range(NZ):
            for x in range(NX):
                for k in range(NK):
                    ty, tz, tx, tk = where(y, z, x, k)
                    src = ((y * NZ + z) * NX + x) * NK + k
                    dst = ((ty % NY * NZ + tz % NZ) * NX + tx % NX) * NK + tk % NK
                    pairs.append((src, dst))
    return pairs


def send(a, where):
    return lax.ppermute(a, AXES, route(where))


def first_ring(d):
    return lambda y, z, x, k: (y, z, x + d, k) if k == 0 else (y + d, z, x, k)


def second_ring(d):
    return lambda y, z, x, k: (y + d, z, x, k) if k == 0 else (y, z, x + d, k)


def z_ring(d):
    return lambda y, z, x, k: (y, z + d, x, k)


def y_ring(d):
    return lambda y, z, x, k: (y + d, z, x, k)


def other_core(y, z, x, k):
    return (y, z, x, 1 - k)


def to_left_owner(y, z, x, k):
    return (y, z ^ (2 * x + k), (y - z) % NY, z // 4)


def gather(piece):
    half = piece.shape[0] // 2
    left = [send(piece, to_left_owner)]
    minus, plus = send(piece, first_ring(1)), send(piece, first_ring(-1))
    across = send(piece, first_ring(2))
    mine = jnp.stack([piece, minus, plus, across])
    left += [send(left[0], z_ring(1)), send(left[0], z_ring(-1))]
    m, p = send(mine, second_ring(1)), send(mine, second_ring(-1))
    theirs = [send(mine, other_core)]
    left += [send(left[1], z_ring(1)), send(left[2], z_ring(-1))]
    fm, fp = send(m[:2], second_ring(1)), send(p[2:], second_ring(-1))
    theirs += [send(m, other_core), send(p, other_core)]
    left += [send(left[3], z_ring(1)), send(left[4], z_ring(-1))]
    theirs += [send(fm, other_core), send(fp, other_core)]
    left += [send(left[5][:half], z_ring(1)), send(left[6][half:], z_ring(-1))]
    return left, [mine, m, p, fm, fp], theirs


DIMS = (((1,), (1,)), ((), ()))


def contract(a, b):
    return lax.dot_general(a, b, DIMS, preferred_element_type=jnp.float32)


def columns(share, width):
    return pl.ds(pl.multiple_of(share * width, width), width)


def most_kernel(*refs):
    left, refs = refs[:7], refs[7:]
    bundles, refs = (refs[:5], refs[5:10]), refs[10:]
    (valence_sums, conduction_sums, last), (lv, lc, rv, rc) = refs[:3], refs[3:]
    y, z, x, k = (lax.axis_index(a) for a in AXES)
    rows = left[0].shape[0]
    nv = rv.shape[1] // (NX * NK)
    nc = rc.shape[1] // (NX * NK)
    zb = 4 * k + ((y - x) & 3)
    last_share = ((z + 4) & 7) ^ zb
    for ref, far in zip(left, (0, -1, 1, -2, 2, -3, 3)):
        share = ((z + far) & 7) ^ zb
        lv[:, columns(share, nv)] = ref[:, :nv]
        lc[:, columns(share, nc)] = ref[:, nv:]
    lv[:, columns(last_share, nv)] = jnp.zeros((rows, nv), lv.dtype)
    lc[:, columns(last_share, nc)] = jnp.zeros((rows, nc), lc.dtype)
    for bundle, core in zip(bundles, (k, 1 - k)):
        for i, a in enumerate(RING):
            for j, b in enumerate(RING):
                if i < 3:
                    ref = bundle[i].at[j]
                else:
                    ref = bundle[3 + j // 2].at[j % 2]
                dy = jnp.where(core == 0, a, b) & 3
                dx = jnp.where(core == 0, b, a)
                share = 2 * ((x + dx) & 3) + core
                here = pl.ds(pl.multiple_of(dy * rows, rows), rows)
                rv[here, columns(share, nv)] = ref[:, :nv]
                rc[here, columns(share, nc)] = ref[:, nv:]
    last[:, :nv] = rv[:, columns(last_share, nv)]
    last[:, nv:] = rc[:, columns(last_share, nc)]
    for a in range(NY):
        here = pl.ds(a * rows, rows)
        valence_sums[here, :] = contract(lv[...], rv[here, :])
        conduction_sums[here, :] = contract(lc[...], rc[here, :])


def rest_kernel(upper, lower, last, valence_sums, conduction_sums, *outs, nv):
    z = lax.axis_index("z")
    rows = outs[0].shape[0]
    half = rows // 2
    for e, out in enumerate(outs):
        here = pl.ds(pl.multiple_of(((e + z) & 3) * rows, rows), rows)
        right = last[here, :]
        gv, gc = valence_sums[here, :], conduction_sums[here, :]
        for at, ref in ((0, upper), (half, lower)):
            part = slice(at, at + half)
            out[part, :] = (gv[part] + contract(ref[:, :nv], right[:, :nv])) * (
                gc[part] + contract(ref[:, nv:], right[:, nv:])
            )


def gram_tiles(left, mine, theirs, nv):
    rows, width = left[0].shape
    nc = width - nv
    shares = NX * NK
    vmem = pl.BlockSpec(memory_space=pltpu.VMEM)
    sums = pl.pallas_call(
        most_kernel,
        out_shape=[jax.ShapeDtypeStruct((NY * rows, rows), jnp.float32)] * 2
        + [jax.ShapeDtypeStruct((NY * rows, width), jnp.bfloat16)],
        in_specs=[vmem] * 17,
        out_specs=[vmem] * 3,
        scratch_shapes=[
            pltpu.VMEM((rows, shares * nv), jnp.bfloat16),
            pltpu.VMEM((rows, shares * nc), jnp.bfloat16),
            pltpu.VMEM((NY * rows, shares * nv), jnp.bfloat16),
            pltpu.VMEM((NY * rows, shares * nc), jnp.bfloat16),
        ],
        compiler_params=pltpu.CompilerParams(vmem_limit_bytes=24 << 20),
        name="most",
    )(*left[:7], *mine, *theirs)
    return pl.pallas_call(
        functools.partial(rest_kernel, nv=nv),
        out_shape=[jax.ShapeDtypeStruct((rows, rows), jnp.float32)] * NY,
        in_specs=[vmem] * 5,
        out_specs=[vmem] * NY,
        compiler_params=pltpu.CompilerParams(vmem_limit_bytes=12 << 20),
        name="rest",
    )(*left[7:], sums[2], sums[0], sums[1])


def place_kernel(*refs):
    parts, out, sems = refs[:NY], refs[NY], refs[NY + 1]
    y, x = lax.axis_index("y"), lax.axis_index("x")
    rows = parts[0].shape[0]
    copies = []
    for e, ref in enumerate(parts):
        here = pl.ds(pl.multiple_of(((y + e - x) & 3) * rows, rows), rows)
        copies.append(pltpu.make_async_copy(ref, out.at[here, :], sems.at[e]))
        copies[-1].start()
    for copy in copies:
        copy.wait()


def place(parts):
    rows, width = parts[0].shape
    anywhere = pl.BlockSpec(memory_space=pl.ANY)
    return pl.pallas_call(
        place_kernel,
        out_shape=jax.ShapeDtypeStruct((NY * rows, width), jnp.float32),
        in_specs=[anywhere] * NY,
        out_specs=anywhere,
        scratch_shapes=[pltpu.SemaphoreType.DMA((NY,))],
        compiler_params=pltpu.CompilerParams(vmem_limit_bytes=1 << 20),
        name="place",
    )(*parts)


def tiles_of(valence, conduction, point_index):
    n_row = NY * NZ
    y, z = lax.axis_index("y"), lax.axis_index("z")
    my_row = y * NZ + z
    my_block = ((y - z) & 3) * NZ + z
    cells = valence.shape[0]
    blocks = point_index.reshape(n_row, -1)
    per_block = blocks.shape[1]
    owners = blocks // cells
    offsets = blocks - owners * cells
    at = jnp.arange(per_block, dtype=jnp.int32)
    earlier = (at[:, None] < at[None, :]).astype(jnp.bfloat16)
    owned = owners == my_row
    own_owner = lax.dynamic_index_in_dim(owners, my_block, 0, keepdims=False)
    own_is = own_owner[None, :] == jnp.arange(n_row, dtype=jnp.int32)[:, None]
    counts = jnp.dot(
        jnp.concatenate([owned, own_is]).astype(jnp.bfloat16),
        earlier,
        preferred_element_type=jnp.float32,
    ).astype(jnp.int32)
    ranks, own_ranks = counts[:n_row], counts[n_row:]
    slots = jnp.arange(CAP, dtype=jnp.int32)
    picked = owned[:, None, :] & (ranks[:, None, :] == slots[None, :, None])
    source = jnp.sum(jnp.where(picked, offsets[:, None, :], 0), axis=2)
    order = jnp.array(
        [((d // NZ - d % NZ) % NY) * NZ + d % NZ for d in range(n_row)], dtype=jnp.int32
    )
    source = source[order].reshape(-1)
    flat_slot = own_owner * CAP + jnp.sum(jnp.where(own_is, own_ranks, 0), axis=0)

    outgoing = jnp.concatenate([valence[source], conduction[source]], axis=1)
    got = lax.all_to_all(
        outgoing.reshape(n_row, CAP, -1), ("y", "z"), split_axis=0, concat_axis=0, tiled=True
    )
    piece = got.reshape(n_row * CAP, -1)[flat_slot]

    left, mine, theirs = gather(piece)
    tiles = gram_tiles(left, mine, theirs, valence.shape[1])
    parts = [tiles[0]] + [send(tiles[(-e) % NY], y_ring(-e)) for e in range(1, NY)]
    return place(parts)


def solution(mesh):
    fine = Mesh(mesh.devices.reshape(NY, NZ, NX, NK), AXES)
    row, col = ("y", "z"), ("x", "core")
    return jax.shard_map(
        tiles_of,
        mesh=fine,
        in_specs=(P(row, col), P(row, col), P()),
        out_specs=P(col, row),
        check_vma=False,
    )
```

```python
import functools

import jax
import jax.numpy as jnp
from jax import lax
from jax.experimental import pallas as pl
from jax.experimental.pallas import tpu as pltpu
from jax.sharding import Mesh, PartitionSpec as P


NY, NZ, NX, NK = 4, 8, 4, 2
AXES = ("y", "z", "x", "core")
CAP = 16
RING = (0, -1, 1, 2)


def route(where):
    pairs = []
    for y in range(NY):
        for z in range(NZ):
            for x in range(NX):
                for k in range(NK):
                    ty, tz, tx, tk = where(y, z, x, k)
                    src = ((y * NZ + z) * NX + x) * NK + k
                    dst = ((ty % NY * NZ + tz % NZ) * NX + tx % NX) * NK + tk % NK
                    pairs.append((src, dst))
    return pairs


def send(a, where):
    return lax.ppermute(a, AXES, route(where))


def first_ring(d):
    return lambda y, z, x, k: (y, z, x + d, k) if k == 0 else (y + d, z, x, k)


def second_ring(d):
    return lambda y, z, x, k: (y + d, z, x, k) if k == 0 else (y, z, x + d, k)


def z_ring(d):
    return lambda y, z, x, k: (y, z + d, x, k)


def y_ring(d):
    return lambda y, z, x, k: (y + d, z, x, k)


def other_core(y, z, x, k):
    return (y, z, x, 1 - k)


def held_block(y, z):
    return (y - z) & 3


def to_left_owner(y, z, x, k):
    block = held_block(y, z)
    return (block + z, z ^ (2 * x + k), block, z // 4)


def gather(piece):
    half = piece.shape[0] // 2
    left = [send(piece, to_left_owner)]
    across = send(piece, first_ring(2))
    minus, plus = send(piece, first_ring(1)), send(piece, first_ring(-1))
    mine = jnp.stack([piece, minus, plus, across])
    left += [send(left[0], z_ring(1)), send(left[0], z_ring(-1))]
    m, p = send(mine, second_ring(1)), send(mine, second_ring(-1))
    left += [send(left[1], z_ring(1)), send(left[2], z_ring(-1))]
    fm, fp = send(m[:2], second_ring(1)), send(p[2:], second_ring(-1))
    theirs = [send(jnp.concatenate([mine, m, p]), other_core)]
    left += [send(left[3], z_ring(1)), send(left[4], z_ring(-1))]
    theirs += [send(jnp.concatenate([fm, fp]), other_core)]
    left += [send(left[5][:half], z_ring(1)), send(left[6][half:], z_ring(-1))]
    return left, [mine, m, p, fm, fp], theirs


DIMS = (((1,), (1,)), ((), ()))


def contract(a, b):
    return lax.dot_general(a, b, DIMS, preferred_element_type=jnp.float32)


def columns(share, width):
    return pl.ds(pl.multiple_of(share * width, width), width)


def most_kernel(*refs):
    left, refs = refs[:7], refs[7:]
    (mine, theirs), refs = (refs[:5], refs[5:7]), refs[7:]
    (valence_sums, conduction_sums, last), (lv, lc, rv, rc) = refs[:3], refs[3:]
    y, z, x, k = (lax.axis_index(a) for a in AXES)
    rows = left[0].shape[0]
    nv = rv.shape[1] // (NX * NK)
    nc = rc.shape[1] // (NX * NK)
    zb = 4 * k + ((y - x) & 3)
    last_share = ((z + 4) & 7) ^ zb
    for ref, far in zip(left, (0, -1, 1, -2, 2, -3, 3)):
        share = ((z + far) & 7) ^ zb
        lv[:, columns(share, nv)] = ref[:, :nv]
        lc[:, columns(share, nc)] = ref[:, nv:]
    lv[:, columns(last_share, nv)] = jnp.zeros((rows, nv), lv.dtype)
    lc[:, columns(last_share, nc)] = jnp.zeros((rows, nc), lc.dtype)
    for i, a in enumerate(RING):
        for j, b in enumerate(RING):
            own = mine[i].at[j] if i < 3 else mine[3 + j // 2].at[j % 2]
            other = theirs[0].at[4 * i + j] if i < 3 else theirs[1].at[j]
            for ref, core in ((own, k), (other, 1 - k)):
                dy = jnp.where(core == 0, a, b)
                dx = jnp.where(core == 0, b, a)
                block = held_block(y + dy, z)
                share = 2 * ((x + dx) & 3) + core
                here = pl.ds(pl.multiple_of(block * rows, rows), rows)
                rv[here, columns(share, nv)] = ref[:, :nv]
                rc[here, columns(share, nc)] = ref[:, nv:]
    last[:, :nv] = rv[:, columns(last_share, nv)]
    last[:, nv:] = rc[:, columns(last_share, nc)]
    for a in range(NY):
        here = pl.ds(a * rows, rows)
        valence_sums[here, :] = contract(lv[...], rv[here, :])
        conduction_sums[here, :] = contract(lc[...], rc[here, :])


def rest_kernel(upper, lower, last, valence_sums, conduction_sums, *outs, nv):
    y = lax.axis_index("y")
    rows = outs[0].shape[0]
    half = rows // 2
    for e, out in enumerate(outs):
        here = pl.ds(pl.multiple_of(((e + y) & 3) * rows, rows), rows)
        right = last[here, :]
        gv, gc = valence_sums[here, :], conduction_sums[here, :]
        for at, ref in ((0, upper), (half, lower)):
            part = slice(at, at + half)
            out[part, :] = (gv[part] + contract(ref[:, :nv], right[:, :nv])) * (
                gc[part] + contract(ref[:, nv:], right[:, nv:])
            )


def gram_tiles(left, mine, theirs, nv):
    rows, width = left[0].shape
    nc = width - nv
    shares = NX * NK
    vmem = pl.BlockSpec(memory_space=pltpu.VMEM)
    sums = pl.pallas_call(
        most_kernel,
        out_shape=[jax.ShapeDtypeStruct((NY * rows, rows), jnp.float32)] * 2
        + [jax.ShapeDtypeStruct((NY * rows, width), jnp.bfloat16)],
        in_specs=[vmem] * 14,
        out_specs=[vmem] * 3,
        scratch_shapes=[
            pltpu.VMEM((rows, shares * nv), jnp.bfloat16),
            pltpu.VMEM((rows, shares * nc), jnp.bfloat16),
            pltpu.VMEM((NY * rows, shares * nv), jnp.bfloat16),
            pltpu.VMEM((NY * rows, shares * nc), jnp.bfloat16),
        ],
        compiler_params=pltpu.CompilerParams(vmem_limit_bytes=24 << 20),
        name="most",
    )(*left[:7], *mine, *theirs)
    return pl.pallas_call(
        functools.partial(rest_kernel, nv=nv),
        out_shape=[jax.ShapeDtypeStruct((rows, rows), jnp.float32)] * NY,
        in_specs=[vmem] * 5,
        out_specs=[vmem] * NY,
        compiler_params=pltpu.CompilerParams(vmem_limit_bytes=12 << 20),
        name="rest",
    )(*left[7:], sums[2], sums[0], sums[1])


def place_kernel(*refs):
    parts, out, sems = refs[:NY], refs[NY], refs[NY + 1]
    y, x = lax.axis_index("y"), lax.axis_index("x")
    rows = parts[0].shape[0]
    copies = []
    for e, ref in enumerate(parts):
        here = pl.ds(pl.multiple_of(((y + e - x) & 3) * rows, rows), rows)
        copies.append(pltpu.make_async_copy(ref, out.at[here, :], sems.at[e]))
        copies[-1].start()
    for copy in copies:
        copy.wait()


def place(parts):
    rows, width = parts[0].shape
    anywhere = pl.BlockSpec(memory_space=pl.ANY)
    return pl.pallas_call(
        place_kernel,
        out_shape=jax.ShapeDtypeStruct((NY * rows, width), jnp.float32),
        in_specs=[anywhere] * NY,
        out_specs=anywhere,
        scratch_shapes=[pltpu.SemaphoreType.DMA((NY,))],
        compiler_params=pltpu.CompilerParams(vmem_limit_bytes=1 << 20),
        name="place",
    )(*parts)


def pick_kernel(points, valence, conduction, outgoing, wanted, lift, val, cond, sems):
    copies = [
        pltpu.make_async_copy(valence, val, sems.at[0]),
        pltpu.make_async_copy(conduction, cond, sems.at[1]),
    ]
    for copy in copies:
        copy.start()
    n_row = NY * NZ
    cells = val.shape[0]
    width = val.shape[1]
    bits = cells.bit_length() - 1
    y, z = lax.axis_index("y"), lax.axis_index("z")
    lanes = points.shape[1]
    per_block = points.shape[0] // n_row * lanes

    def block_rows(first, count):
        parts = [points[pl.ds(first + i, count, stride=2), :] for i in range(2)]
        return jnp.concatenate(parts, axis=1)

    def iota(shape, dim):
        return lax.broadcasted_iota(jnp.int32, shape, dim)

    cell = block_rows(0, n_row)
    offset = (cell & (cells - 1)).astype(jnp.float32)
    owned = (cell >> bits) == y * NZ + z
    mine = 2 * (held_block(y, z) * NZ + z)
    own_owner = jnp.concatenate([points[pl.ds(mine + i, 1), :] for i in range(2)], axis=1) >> bits
    own_is = own_owner == iota((n_row, per_block), 0)
    earlier = iota((per_block, per_block), 0) < iota((per_block, per_block), 1)
    masks = jnp.concatenate([owned.astype(jnp.float32), own_is.astype(jnp.float32)])
    counts = jnp.dot(
        masks.astype(jnp.bfloat16),
        earlier.astype(jnp.float32).astype(jnp.bfloat16),
        preferred_element_type=jnp.float32,
    )
    rank = jnp.where(owned, counts[:n_row], -1.0)
    own_rank = jnp.sum(jnp.where(own_is, counts[n_row:], 0.0), axis=0, keepdims=True)
    own_slot = own_owner * CAP + own_rank.astype(jnp.int32)
    wanted[...] = (
        (iota((n_row * CAP, per_block), 0) == own_slot).astype(jnp.float32).astype(jnp.bfloat16)
    )
    slot = iota((CAP, per_block), 0).astype(jnp.float32)
    all_cells = iota((CAP, cells), 1)
    for d in range(n_row):
        b = held_block(d // NZ, d % NZ) * NZ + d % NZ
        here = rank[b : b + 1] == slot
        at = jnp.sum(jnp.where(here, offset[b : b + 1], 0.0), axis=1, keepdims=True)
        hot = (all_cells == at.astype(jnp.int32)).astype(jnp.float32)
        lift[pl.ds(d * CAP, CAP), :] = hot.astype(jnp.bfloat16)
    for copy in copies:
        copy.wait()
    for ref, columns_of in ((val, slice(0, width)), (cond, slice(width, None))):
        outgoing[:, columns_of] = jnp.dot(
            lift[...], ref[...], preferred_element_type=jnp.float32
        ).astype(jnp.bfloat16)


def pick(points, valence, conduction):
    vmem, anywhere = (pl.BlockSpec(memory_space=m) for m in (pltpu.VMEM, pl.ANY))
    n_row = NY * NZ
    width = valence.shape[1] + conduction.shape[1]
    return pl.pallas_call(
        pick_kernel,
        out_shape=[
            jax.ShapeDtypeStruct((n_row * CAP, width), jnp.bfloat16),
            jax.ShapeDtypeStruct((n_row * CAP, points.size // n_row), jnp.bfloat16),
        ],
        in_specs=[vmem, anywhere, anywhere],
        out_specs=[vmem] * 2,
        scratch_shapes=[
            pltpu.VMEM((n_row * CAP, valence.shape[0]), jnp.bfloat16),
            pltpu.VMEM(valence.shape, jnp.bfloat16),
            pltpu.VMEM(conduction.shape, jnp.bfloat16),
            pltpu.SemaphoreType.DMA((2,)),
        ],
        compiler_params=pltpu.CompilerParams(vmem_limit_bytes=20 << 20),
        name="pick",
    )(points, *(pltpu.with_memory_space_constraint(a, pltpu.HBM) for a in (valence, conduction)))


def compact_kernel(wanted, got, piece):
    piece[...] = lax.dot_general(
        wanted[...], got[...], (((0,), (0,)), ((), ())), preferred_element_type=jnp.float32
    ).astype(jnp.bfloat16)


def compact(wanted, got):
    vmem = pl.BlockSpec(memory_space=pltpu.VMEM)
    return pl.pallas_call(
        compact_kernel,
        out_shape=jax.ShapeDtypeStruct((wanted.shape[1], got.shape[1]), jnp.bfloat16),
        in_specs=[vmem] * 2,
        out_specs=vmem,
        compiler_params=pltpu.CompilerParams(vmem_limit_bytes=4 << 20),
        name="compact",
    )(wanted, got)


def tiles_of(valence, conduction, point_index):
    n_row = NY * NZ
    outgoing, wanted = pick(point_index.reshape(-1, 128), valence, conduction)
    got = lax.all_to_all(
        outgoing.reshape(n_row, CAP, -1), ("y", "z"), split_axis=0, concat_axis=0, tiled=True
    )
    piece = compact(wanted, got.reshape(n_row * CAP, -1))

    left, mine, theirs = gather(piece)
    tiles = gram_tiles(left, mine, theirs, valence.shape[1])
    parts = [tiles[0]]
    for e in range(1, NY):
        parts.append(send(tiles[(-e) % NY], y_ring(-e)))
    return place(parts)


def solution(mesh):
    fine = Mesh(mesh.devices.reshape(NY, NZ, NX, NK), AXES)
    row, col = ("y", "z"), ("x", "core")
    return jax.shard_map(
        tiles_of,
        mesh=fine,
        in_specs=(P(row, col), P(row, col), P()),
        out_specs=P(col, row),
        check_vma=False,
    )
```

```python
import functools

import jax
import jax.numpy as jnp
from jax import lax
from jax.experimental import pallas as pl
from jax.experimental.pallas import tpu as pltpu
from jax.sharding import Mesh, PartitionSpec as P


NY, NZ, NX, NK = 4, 8, 4, 2
AXES = ("y", "z", "x", "core")
CAP = 16
RING = (0, -1, 1, 2)


def route(where):
    pairs = []
    for y in range(NY):
        for z in range(NZ):
            for x in range(NX):
                for k in range(NK):
                    ty, tz, tx, tk = where(y, z, x, k)
                    src = ((y * NZ + z) * NX + x) * NK + k
                    dst = ((ty % NY * NZ + tz % NZ) * NX + tx % NX) * NK + tk % NK
                    pairs.append((src, dst))
    return pairs


def send(a, where):
    return lax.ppermute(a, AXES, route(where))


def first_ring(d):
    return lambda y, z, x, k: (y, z, x + d, k) if k == 0 else (y + d, z, x, k)


def second_ring(d):
    return lambda y, z, x, k: (y + d, z, x, k) if k == 0 else (y, z, x + d, k)


def z_ring(d):
    return lambda y, z, x, k: (y, z + d, x, k)


def y_ring(d):
    return lambda y, z, x, k: (y + d, z, x, k)


def other_core(y, z, x, k):
    return (y, z, x, 1 - k)


def held_block(y, z):
    return (y - z) & 3


def to_left_owner(y, z, x, k):
    block = held_block(y, z)
    return (block + z, z ^ (2 * x + k), block, z // 4)


def gather(piece):
    half = piece.shape[0] // 2
    left = [send(piece, to_left_owner)]
    across = send(piece, first_ring(2))
    minus, plus = send(piece, first_ring(1)), send(piece, first_ring(-1))
    mine = jnp.stack([piece, minus, plus, across])
    left += [send(left[0], z_ring(1)), send(left[0], z_ring(-1))]
    m, p = send(mine, second_ring(1)), send(mine, second_ring(-1))
    left += [send(left[1], z_ring(1)), send(left[2], z_ring(-1))]
    fm, fp = send(m[:2], second_ring(1)), send(p[2:], second_ring(-1))
    theirs = [send(jnp.concatenate([mine, m, p]), other_core)]
    left += [send(left[3], z_ring(1)), send(left[4], z_ring(-1))]
    theirs += [send(jnp.concatenate([fm, fp]), other_core)]
    left += [send(left[5][:half], z_ring(1)), send(left[6][half:], z_ring(-1))]
    return left, [mine, m, p, fm, fp], theirs


DIMS = (((1,), (1,)), ((), ()))


def contract(a, b):
    return lax.dot_general(a, b, DIMS, preferred_element_type=jnp.float32)


def columns(share, width):
    return pl.ds(pl.multiple_of(share * width, width), width)


def most_kernel(*refs):
    left, refs = refs[:7], refs[7:]
    (mine, theirs), refs = (refs[:5], refs[5:7]), refs[7:]
    (valence_sums, conduction_sums, last), (lv, lc, rv, rc) = refs[:3], refs[3:]
    y, z, x, k = (lax.axis_index(a) for a in AXES)
    rows = left[0].shape[0]
    nv = rv.shape[1] // (NX * NK)
    nc = rc.shape[1] // (NX * NK)
    zb = 4 * k + ((y - x) & 3)
    last_share = ((z + 4) & 7) ^ zb
    for ref, far in zip(left, (0, -1, 1, -2, 2, -3, 3)):
        share = ((z + far) & 7) ^ zb
        lv[:, columns(share, nv)] = ref[:, :nv]
        lc[:, columns(share, nc)] = ref[:, nv:]
    lv[:, columns(last_share, nv)] = jnp.zeros((rows, nv), lv.dtype)
    lc[:, columns(last_share, nc)] = jnp.zeros((rows, nc), lc.dtype)
    for i, a in enumerate(RING):
        for j, b in enumerate(RING):
            own = mine[i].at[j] if i < 3 else mine[3 + j // 2].at[j % 2]
            other = theirs[0].at[4 * i + j] if i < 3 else theirs[1].at[j]
            for ref, core in ((own, k), (other, 1 - k)):
                dy = jnp.where(core == 0, a, b)
                dx = jnp.where(core == 0, b, a)
                block = held_block(y + dy, z)
                share = 2 * ((x + dx) & 3) + core
                here = pl.ds(pl.multiple_of(block * rows, rows), rows)
                rv[here, columns(share, nv)] = ref[:, :nv]
                rc[here, columns(share, nc)] = ref[:, nv:]
    last[:, :nv] = rv[:, columns(last_share, nv)]
    last[:, nv:] = rc[:, columns(last_share, nc)]
    for a in range(NY):
        here = pl.ds(a * rows, rows)
        valence_sums[here, :] = contract(lv[...], rv[here, :])
        conduction_sums[here, :] = contract(lc[...], rc[here, :])


def rest_kernel(upper, lower, last, valence_sums, conduction_sums, *outs, nv):
    y = lax.axis_index("y")
    rows = outs[0].shape[0]
    half = rows // 2
    for e, out in enumerate(outs):
        here = pl.ds(pl.multiple_of(((e + y) & 3) * rows, rows), rows)
        right = last[here, :]
        gv, gc = valence_sums[here, :], conduction_sums[here, :]
        for at, ref in ((0, upper), (half, lower)):
            part = slice(at, at + half)
            out[part, :] = (gv[part] + contract(ref[:, :nv], right[:, :nv])) * (
                gc[part] + contract(ref[:, nv:], right[:, nv:])
            )


def gram_tiles(left, mine, theirs, nv):
    rows, width = left[0].shape
    nc = width - nv
    shares = NX * NK
    vmem = pl.BlockSpec(memory_space=pltpu.VMEM)
    sums = pl.pallas_call(
        most_kernel,
        out_shape=[jax.ShapeDtypeStruct((NY * rows, rows), jnp.float32)] * 2
        + [jax.ShapeDtypeStruct((NY * rows, width), jnp.bfloat16)],
        in_specs=[vmem] * 14,
        out_specs=[vmem] * 3,
        scratch_shapes=[
            pltpu.VMEM((rows, shares * nv), jnp.bfloat16),
            pltpu.VMEM((rows, shares * nc), jnp.bfloat16),
            pltpu.VMEM((NY * rows, shares * nv), jnp.bfloat16),
            pltpu.VMEM((NY * rows, shares * nc), jnp.bfloat16),
        ],
        compiler_params=pltpu.CompilerParams(vmem_limit_bytes=24 << 20),
        name="most",
    )(*left[:7], *mine, *theirs)
    return pl.pallas_call(
        functools.partial(rest_kernel, nv=nv),
        out_shape=[jax.ShapeDtypeStruct((rows, rows), jnp.float32)] * NY,
        in_specs=[vmem] * 5,
        out_specs=[vmem] * NY,
        compiler_params=pltpu.CompilerParams(vmem_limit_bytes=12 << 20),
        name="rest",
    )(*left[7:], sums[2], sums[0], sums[1])


def place_kernel(*refs):
    parts, out, sems = refs[:NY], refs[NY], refs[NY + 1]
    y, x = lax.axis_index("y"), lax.axis_index("x")
    rows = parts[0].shape[0]
    copies = []
    for e, ref in enumerate(parts):
        here = pl.ds(pl.multiple_of(((y + e - x) & 3) * rows, rows), rows)
        copies.append(pltpu.make_async_copy(ref, out.at[here, :], sems.at[e]))
        copies[-1].start()
    for copy in copies:
        copy.wait()


def place(parts):
    rows, width = parts[0].shape
    anywhere = pl.BlockSpec(memory_space=pl.ANY)
    return pl.pallas_call(
        place_kernel,
        out_shape=jax.ShapeDtypeStruct((NY * rows, width), jnp.float32),
        in_specs=[anywhere] * NY,
        out_specs=anywhere,
        scratch_shapes=[pltpu.SemaphoreType.DMA((NY,))],
        compiler_params=pltpu.CompilerParams(vmem_limit_bytes=1 << 20),
        name="place",
    )(*parts)


def pick_kernel(points, valence, conduction, outgoing, wanted, lift, val, cond, sems):
    copies = [
        pltpu.make_async_copy(valence, val, sems.at[0]),
        pltpu.make_async_copy(conduction, cond, sems.at[1]),
    ]
    for copy in copies:
        copy.start()
    n_row = NY * NZ
    cells = val.shape[0]
    width = val.shape[1]
    bits = cells.bit_length() - 1
    y, z = lax.axis_index("y"), lax.axis_index("z")
    lanes = points.shape[1]
    per_block = points.shape[0] // n_row * lanes

    def block_rows(first, count):
        parts = [points[pl.ds(first + i, count, stride=2), :] for i in range(2)]
        return jnp.concatenate(parts, axis=1)

    def iota(shape, dim):
        return lax.broadcasted_iota(jnp.int32, shape, dim)

    cell = block_rows(0, n_row)
    offset = (cell & (cells - 1)).astype(jnp.float32)
    owned = (cell >> bits) == y * NZ + z
    mine = 2 * (held_block(y, z) * NZ + z)
    own_owner = jnp.concatenate([points[pl.ds(mine + i, 1), :] for i in range(2)], axis=1) >> bits
    own_is = own_owner == iota((n_row, per_block), 0)
    earlier = iota((per_block, per_block), 0) < iota((per_block, per_block), 1)
    masks = jnp.concatenate([owned.astype(jnp.float32), own_is.astype(jnp.float32)])
    counts = jnp.dot(
        masks.astype(jnp.bfloat16),
        earlier.astype(jnp.float32).astype(jnp.bfloat16),
        preferred_element_type=jnp.float32,
    )
    rank = jnp.where(owned, counts[:n_row], -1.0)
    own_rank = jnp.sum(jnp.where(own_is, counts[n_row:], 0.0), axis=0, keepdims=True)
    own_slot = own_owner * CAP + own_rank.astype(jnp.int32)
    wanted[...] = (
        (iota((n_row * CAP, per_block), 0) == own_slot).astype(jnp.float32).astype(jnp.bfloat16)
    )
    slot = iota((CAP, per_block), 0).astype(jnp.float32)
    all_cells = iota((CAP, cells), 1)
    per_group = n_row // 4
    for first in range(0, n_row, per_group):
        for d in range(first, first + per_group):
            b = held_block(d // NZ, d % NZ) * NZ + d % NZ
            here = rank[b : b + 1] == slot
            at = jnp.sum(jnp.where(here, offset[b : b + 1], 0.0), axis=1, keepdims=True)
            hot = (all_cells == at.astype(jnp.int32)).astype(jnp.float32)
            lift[pl.ds(d * CAP, CAP), :] = hot.astype(jnp.bfloat16)
        if first == 0:
            for copy in copies:
                copy.wait()
        rows = pl.ds(first * CAP, per_group * CAP)
        for ref, columns_of in ((val, slice(0, width)), (cond, slice(width, None))):
            outgoing[rows, columns_of] = jnp.dot(
                lift[rows, :], ref[...], preferred_element_type=jnp.float32
            ).astype(jnp.bfloat16)


def pick(points, valence, conduction):
    vmem, anywhere = (pl.BlockSpec(memory_space=m) for m in (pltpu.VMEM, pl.ANY))
    n_row = NY * NZ
    width = valence.shape[1] + conduction.shape[1]
    return pl.pallas_call(
        pick_kernel,
        out_shape=[
            jax.ShapeDtypeStruct((n_row * CAP, width), jnp.bfloat16),
            jax.ShapeDtypeStruct((n_row * CAP, points.size // n_row), jnp.bfloat16),
        ],
        in_specs=[vmem, anywhere, anywhere],
        out_specs=[vmem] * 2,
        scratch_shapes=[
            pltpu.VMEM((n_row * CAP, valence.shape[0]), jnp.bfloat16),
            pltpu.VMEM(valence.shape, jnp.bfloat16),
            pltpu.VMEM(conduction.shape, jnp.bfloat16),
            pltpu.SemaphoreType.DMA((2,)),
        ],
        compiler_params=pltpu.CompilerParams(vmem_limit_bytes=20 << 20),
        name="pick",
    )(points, *(pltpu.with_memory_space_constraint(a, pltpu.HBM) for a in (valence, conduction)))


def compact_kernel(wanted, got, piece):
    piece[...] = lax.dot_general(
        wanted[...], got[...], (((0,), (0,)), ((), ())), preferred_element_type=jnp.float32
    ).astype(jnp.bfloat16)


def compact(wanted, got):
    vmem = pl.BlockSpec(memory_space=pltpu.VMEM)
    return pl.pallas_call(
        compact_kernel,
        out_shape=jax.ShapeDtypeStruct((wanted.shape[1], got.shape[1]), jnp.bfloat16),
        in_specs=[vmem] * 2,
        out_specs=vmem,
        compiler_params=pltpu.CompilerParams(vmem_limit_bytes=4 << 20),
        name="compact",
    )(wanted, got)


def tiles_of(valence, conduction, point_index):
    n_row = NY * NZ
    outgoing, wanted = pick(point_index.reshape(-1, 128), valence, conduction)
    got = lax.all_to_all(
        outgoing.reshape(n_row, CAP, -1), ("y", "z"), split_axis=0, concat_axis=0, tiled=True
    )
    piece = compact(wanted, got.reshape(n_row * CAP, -1))

    left, mine, theirs = gather(piece)
    tiles = gram_tiles(left, mine, theirs, valence.shape[1])
    parts = [tiles[0]]
    for e in range(1, NY):
        parts.append(send(tiles[(-e) % NY], y_ring(-e)))
    return place(parts)


def solution(mesh):
    fine = Mesh(mesh.devices.reshape(NY, NZ, NX, NK), AXES)
    row, col = ("y", "z"), ("x", "core")
    return jax.shard_map(
        tiles_of,
        mesh=fine,
        in_specs=(P(row, col), P(row, col), P()),
        out_specs=P(col, row),
        check_vma=False,
    )
```
